128 devices in a mesh: member: 4 (over y, x), dp: 32 (over z, core).
Axes of the slice: x: 2, y: 2, z: 16, core: 2. Of those that a mesh axis runs over, the one named last changes fastest.
The devices are a block of a 8x8x16 slice.
Arguments:
- residual: bfloat16 [2048, 3072], P(('member', 'dp')), parts along dimension 0, may hold values from -6 to 6
- upstream: bfloat16 [2048, 3072], P(('member', 'dp')), parts along dimension 0, may hold values from -6 to 6
- gate_weight: bfloat16 [12288, 20480], P('member', 'dp'), parts along dimension 0, may hold values from -0.109375 to 0.109375
- up_weight: bfloat16 [12288, 20480], P('member', 'dp'), parts along dimension 0, may hold values from -0.109375 to 0.109375
- down_weight: bfloat16 [81920, 3072], P(('member', 'dp')), parts along dimension 0, may hold values from -0.0390625 to 0.0390625
- gain: float32 [12288], P('member'), parts along dimension 0, may hold values from 0.25 to 1.75
Outputs:
- grad_residual: bfloat16 [2048, 3072], P(('member', 'dp')), parts along dimension 0
- grad_gate: bfloat16 [12288, 20480], P('member', 'dp'), parts along dimension 0
- grad_up: bfloat16 [12288, 20480], P('member', 'dp'), parts along dimension 0
- grad_down: bfloat16 [81920, 3072], P(('member', 'dp')), parts along dimension 0
- grad_gain: float32 [12288], P('member'), parts along dimension 0
The draws below stay inside these ranges and needn't reach their ends.
There are 4 independent parts, one for each index of `member`. The reference program is written for one: setup_inputs(seed, part) draws one part's arguments, and reference() takes and returns one part's arrays. A program takes and returns all parts, laid end to end along the dimension named above; each array names one. Nothing has to cross between parts.
All inputs are finite; a program needn't handle non-finite values.
Results may differ from the reference program's by a relative error of at most 0.0068.
Values may be sent and summed in bfloat16 or wider, within the bound.
A program may use at most 128 MiB of HBM per device.

```python
import jax
import jax.numpy as jnp
from jax import lax

D = 3072
FF = 20480
TOKENS = 512


def block_scale(stream_key, dims, pieces, smallest, high):
    level, own = 1.0, jax.random.fold_in(stream_key, 6)
    for dim, blocks in pieces:
        steps = jnp.exp(jax.random.uniform(jax.random.fold_in(own, dim), (blocks,), jnp.float32, smallest / len(pieces), high / len(pieces)))
        level = level * jnp.repeat(steps, dims[dim] // blocks).reshape([-1 if axis == dim else 1 for axis in range(len(dims))])
    return level


def normal_values(key, shape, scale, most, split=(), held_as=jnp.bfloat16):
    entries = jax.random.normal(key, shape, jnp.float32) * scale
    if len(split) > 0:
        entries = block_scale(key, shape, split, -0.22, 0.18) * entries
    return jnp.clip(entries, min=-most, max=most).astype(held_as)


def setup_inputs(seed: int = 0, part: int = 0) -> dict:
    key_of = jax.random.split(jax.random.key(seed), 7)
    own_keys = jax.random.split(jax.random.fold_in(key_of[6], part), 7)
    return {
        "residual": normal_values(own_keys[0], (TOKENS, D), 1.0, 6.0, ((0, 32),)),
        "upstream": normal_values(own_keys[1], (TOKENS, D), 1.0, 6.0, ((0, 32),)),
        "gate_weight": normal_values(own_keys[2], (D, FF), D ** -0.5, 0.109375, ((1, 32),)),
        "up_weight": normal_values(own_keys[3], (D, FF), D ** -0.5, 0.109375, ((1, 32),)),
        "down_weight": normal_values(own_keys[4], (FF, D), FF ** -0.5, 0.0390625, ((0, 32),)),
        "gain": jnp.clip(1.0 + 0.15 * jax.random.normal(own_keys[5], (D,), jnp.float32), 0.25, 1.75),
    }


norm_floor = 0.5
gelu_coeff = 0.7978845608
cubic_term = 0.044715

def gelu_parts(gate_out):
    inner = jnp.tanh(gelu_coeff * (gate_out + cubic_term * gate_out * gate_out * gate_out))
    activated = 0.5 * gate_out * (1.0 + inner)
    gelu_slope = 0.5 * (1.0 + inner) + 0.5 * gate_out * (1.0 - inner * inner) * gelu_coeff * (1.0 + 3.0 * cubic_term * gate_out * gate_out)
    return (activated, gelu_slope)

def contract_last(left, right):
    return lax.dot_general(left, right, (((1,), (1,)), ((), ())), preferred_element_type=jnp.float32)

def contract_first(left, right):
    return lax.dot_general(left, right, (((0,), (0,)), ((), ())), preferred_element_type=jnp.float32)

def reference(residual, upstream, gate_weight, up_weight, down_weight, gain):
    widened = residual.astype(jnp.float32)
    norm_scale = lax.rsqrt(lax.optimization_barrier(jnp.mean(widened * widened, axis=1, keepdims=True)) + norm_floor)
    unit_rows = widened * norm_scale
    normed = (unit_rows * gain).astype(jnp.bfloat16)
    gate_out = jnp.dot(normed, gate_weight, preferred_element_type=jnp.float32)
    up_out = jnp.dot(normed, up_weight, preferred_element_type=jnp.float32)
    activated, gelu_slope = gelu_parts(gate_out)
    hidden = (activated * up_out).astype(jnp.bfloat16)
    hidden_grad = contract_last(upstream, down_weight)
    grad_down = contract_first(hidden, upstream).astype(jnp.bfloat16)
    gate_grad = (hidden_grad * up_out * gelu_slope).astype(jnp.bfloat16)
    up_grad = (hidden_grad * activated).astype(jnp.bfloat16)
    grad_gate = contract_first(normed, gate_grad).astype(jnp.bfloat16)
    grad_up = contract_first(normed, up_grad).astype(jnp.bfloat16)
    normed_grad = contract_last(gate_grad, gate_weight) + contract_last(up_grad, up_weight)
    unit_grad = normed_grad * gain
    inner_mean = lax.optimization_barrier(jnp.mean(unit_grad * unit_rows, axis=1, keepdims=True))
    grad_residual = (upstream.astype(jnp.float32) + norm_scale * (unit_grad - unit_rows * inner_mean)).astype(jnp.bfloat16)
    grad_gain = lax.optimization_barrier(jnp.sum(normed_grad * unit_rows, axis=0))
    return (grad_residual, grad_gate, grad_up, grad_down, grad_gain)
```

```python
import functools

import jax
import jax.numpy as jnp
from jax import lax
from jax.experimental import pallas as pl
from jax.experimental.pallas import tpu as pltpu
from jax.sharding import PartitionSpec as P

MESH = pl.DeviceIdType.MESH
F32 = jnp.float32
BF16 = jnp.bfloat16

norm_floor = 0.5
gelu_coeff = 0.7978845608
cubic_term = 0.044715

LANE = 128


def contract_last(left, right):
    return lax.dot_general(left, right, (((1,), (1,)), ((), ())), preferred_element_type=F32)


def contract_first(left, right):
    return lax.dot_general(left, right, (((0,), (0,)), ((), ())), preferred_element_type=F32)


def gelu_parts(gate_out):
    inner = jnp.tanh(gelu_coeff * (gate_out + cubic_term * gate_out * gate_out * gate_out))
    activated = 0.5 * gate_out * (1.0 + inner)
    gelu_slope = 0.5 * (1.0 + inner) + 0.5 * gate_out * (1.0 - inner * inner) * gelu_coeff * (
        1.0 + 3.0 * cubic_term * gate_out * gate_out
    )
    return activated, gelu_slope


def cut(total, most):
    size = most
    while total % size:
        size -= LANE
    return size


def kernel(
    chips, rows, width, units,
    res_ref, ups_ref, gw_ref, uw_ref, dw_ref, gain_ref,
    gres_ref, ggate_ref, gup_ref, gdown_ref, ggain_ref,
    tok, norm, scale, wgu, wd, act, slope, gu, hid,
    pown, pout, pin, sbuf, rbuf, gg, ggin, gring, ggend,
    wsem, own_sem, rs_send, rs_recv, ag_send, ag_recv, x_send, x_recv,
    p_send, p_recv, g_send, g_recv, gx_send, gx_recv,
):
    half = chips // 2
    group = chips // 2
    hw = width // 2
    grows = 2 * group * rows
    blocks = units // LANE

    me = lax.axis_index("dp")
    core = lax.rem(me, 2)
    chip = me // 2
    right = {"dp": lax.rem(chip + 1, chips) * 2 + core}
    left = {"dp": lax.rem(chip + chips - 1, chips) * 2 + core}
    partner = {"dp": me + 1 - 2 * core}
    ahead = (right, left)

    def hops(d, p):
        return half if d == p else half - 1

    def came(d, s):
        return chips - 1 if s == half else (2 * s - 1 if d == 0 else 2 * s)

    def goes(d, s):
        return chips - 1 if s == half else (2 * s if d == 0 else 2 * s - 1)

    def row0(slot, q):
        return (slot // group) * grows + q * group * rows + (slot % group) * rows

    def span(slot, q):
        return pl.ds(row0(slot, q), rows)

    def cols(p):
        return pl.ds(p * hw, hw)

    own = [
        pltpu.make_async_copy(src, tok.at[a, span(0, 0), :], own_sem.at[a])
        for a, src in enumerate((res_ref, ups_ref))
    ]
    for copy in own:
        copy.start()
    loads = []
    for b in range(blocks):
        for k, w in enumerate((gw_ref, uw_ref)):
            loads.append(
                pltpu.make_async_copy(
                    w.at[:, pl.ds(b * LANE, LANE)],
                    wgu.at[:, pl.ds((2 * b + k) * LANE, LANE)],
                    wsem.at[2 * b + k],
                )
            )
    loads.append(pltpu.make_async_copy(dw_ref, wd, wsem.at[2 * blocks]))
    for copy in loads:
        copy.start()

    barrier = pltpu.get_barrier_semaphore()
    for who in (left, right, partner):
        pl.semaphore_signal(barrier, inc=1, device_id=who, device_id_type=MESH)
    pl.semaphore_wait(barrier, 3)

    def ring_copy(a, d, p, s):
        src = 0 if s == 1 else came(d, s - 1)
        return pltpu.make_async_remote_copy(
            src_ref=tok.at[a, span(src, 0), cols(p)],
            dst_ref=tok.at[a, span(came(d, s), 0), cols(p)],
            send_sem=ag_send.at[a, d, p, s - 1],
            recv_sem=ag_recv.at[a, d, p, s - 1],
            device_id=ahead[d],
            device_id_type=MESH,
        )

    def side_copy(a, slot):
        return pltpu.make_async_remote_copy(
            src_ref=tok.at[a, span(slot, 0), :],
            dst_ref=tok.at[a, span(slot, 1), :],
            send_sem=x_send.at[a, slot],
            recv_sem=x_recv.at[a, slot],
            device_id=partner,
            device_id_type=MESH,
        )

    def prep(slot, q):
        at = span(slot, q)
        x = tok[0, at, :].astype(F32)
        sc = lax.rsqrt(jnp.mean(x * x, axis=1, keepdims=True) + norm_floor)
        scale[at, :] = jnp.broadcast_to(sc, (rows, LANE))
        norm[at, :] = ((x * sc) * gain_ref[...]).astype(BF16)

    def gate_up(g, b):
        at = pl.ds(g * grows, grows)
        both = jnp.dot(norm[at, :], wgu[:, pl.ds(2 * b * LANE, 2 * LANE)], preferred_element_type=F32)
        here = pl.ds(b * LANE, LANE)
        up_out = both[:, LANE:]
        activated, gelu_slope = gelu_parts(both[:, :LANE])
        act[:, here] = activated
        slope[:, here] = up_out * gelu_slope
        hid[at, here] = (activated * up_out).astype(BF16)

    def hidden_grad(g, b0, nb):
        at = pl.ds(g * grows, grows)
        hg = contract_last(tok[1, at, :], wd[pl.ds(b0 * LANE, nb * LANE), :])
        for k in range(nb):
            here = pl.ds((b0 + k) * LANE, LANE)
            piece = hg[:, k * LANE : (k + 1) * LANE]
            gu[at, pl.ds(2 * (b0 + k) * LANE, LANE)] = (piece * slope[:, here]).astype(BF16)
            gu[at, pl.ds((2 * (b0 + k) + 1) * LANE, LANE)] = (piece * act[:, here]).astype(BF16)

    pcut = cut(hw, 256)
    per_half = hw // pcut

    def partial(g, p, i):
        at = pl.ds(g * grows, grows)
        c0 = p * hw + i * pcut
        part = contract_last(gu[at, :], wgu[pl.ds(c0, pcut), :])
        unit = tok[0, at, pl.ds(c0, pcut)].astype(F32) * scale[at, 0:1]
        gain_part = jnp.sum(part * unit, axis=0, keepdims=True)
        here = pl.ds(i * pcut, pcut)
        if g == 0:
            gg[p, :, here] = gain_part
        else:
            gg[p, :, here] = gg[p, :, here] + gain_part
        pown[g, p, :, here] = part[: group * rows]
        pout[g, p, :, here] = part[group * rows :].astype(BF16)

    def share(g, p):
        return pltpu.make_async_remote_copy(
            src_ref=pout.at[g, p],
            dst_ref=pin.at[g, p],
            send_sem=p_send.at[g, p],
            recv_sem=p_recv.at[g, p],
            device_id=partner,
            device_id_type=MESH,
        )

    def group_work(g):
        late = []
        b0 = 0
        while b0 < blocks:
            nb = min(2, blocks - b0)
            late.append(functools.partial(hidden_grad, g, b0, nb))
            b0 += nb
        for p in range(2):
            for i in range(per_half):
                late.append(functools.partial(partial, g, p, i))
            late.append(lambda p=p: share(g, p).start())
        return [functools.partial(gate_up, g, b) for b in range(blocks)], late

    own[0].wait()
    for p in range(2):
        for d in range(2):
            ring_copy(0, d, p, 1).start()
    own[1].wait()
    for p in range(2):
        for d in range(2):
            ring_copy(1, d, p, 1).start()
    side_copy(0, 0).start()
    side_copy(1, 0).start()
    prep(0, 0)

    def arrivals(a, s, p):
        for d in range(2):
            if s <= hops(d, p):
                ring_copy(a, d, p, s).wait_recv()
                if s < hops(d, p):
                    ring_copy(a, d, p, s + 1).start()

    def slots_of(s):
        return [0] if s == 0 else ([chips - 1] if s == half else [came(0, s), came(1, s)])

    def sides(a, s):
        for slot in slots_of(s):
            side_copy(a, slot).start()

    waited = set()

    def side_waits(a, s):
        if (a, s) in waited:
            return
        waited.add((a, s))
        for slot in slots_of(s):
            side_copy(a, slot).wait_recv()
            if a == 0:
                prep(slot, 1)

    ready = half // 2

    def once_here(a, work):
        for s in range(ready + 1):
            side_waits(a, s)
        work()

    first_now, first_late = group_work(0)
    first = [functools.partial(once_here, 0, work) for work in first_now]
    first += [functools.partial(once_here, 1, work) for work in first_late]
    places = 4 * (half - ready - 1) + 2
    done = 0
    place = 0
    for s in range(1, half):
        for a in range(2):
            for p in range(2):
                arrivals(a, s, p)
                if p == 0:
                    side_waits(a, s - 1)
                if s > ready:
                    if place == 0:
                        for copy in loads:
                            copy.wait()
                    place += 1
                    upto = min(len(first), -(-len(first) * place // places))
                    for work in first[done:upto]:
                        work()
                    done = upto
            sides(a, s)
            if a == 0:
                for slot in slots_of(s):
                    prep(slot, 0)
    if place == 0:
        for copy in loads:
            copy.wait()
    for work in first[done:]:
        work()
    second_now, second_late = group_work(1)
    for p in range(2):
        arrivals(0, half, p)
    sides(0, half)
    prep(chips - 1, 0)
    side_waits(0, half - 1)
    side_waits(0, half)
    for work in second_now[:-1]:
        work()
    for p in range(2):
        arrivals(1, half, p)
    sides(1, half)
    second_now[-1]()
    side_waits(1, half - 1)
    side_waits(1, half)
    for work in second_late:
        work()

    gain_side = pltpu.make_async_remote_copy(
        src_ref=gg.at[1 - core], dst_ref=ggin, send_sem=gx_send.at[0], recv_sem=gx_recv.at[0],
        device_id=partner, device_id_type=MESH,
    )
    gain_side.start()

    def chain(d, p, i):
        return pltpu.make_async_remote_copy(
            src_ref=sbuf.at[d, p, i - 1], dst_ref=rbuf.at[d, p, i - 1],
            send_sem=rs_send.at[d, p, i - 1], recv_sem=rs_recv.at[d, p, i - 1],
            device_id=ahead[d], device_id_type=MESH,
        )

    def gain_hop(d, i):
        return pltpu.make_async_remote_copy(
            src_ref=gring.at[d, i - 1], dst_ref=gring.at[d, i],
            send_sem=g_send.at[d, i - 1], recv_sem=g_recv.at[d, i - 1],
            device_id=ahead[d], device_id_type=MESH,
        )

    def total(slot, p):
        g = slot // group
        at = pl.ds((slot % group) * rows, rows)
        return pown[g, p, at, :] + pin[g, p, at, :].astype(F32)

    def pass_on(d, p, i):
        count = hops(d, p)
        value = total(goes(d, count + 1 - i), p)
        if i > 1:
            value = value + rbuf[d, p, i - 2].astype(F32)
        sbuf[d, p, i - 1] = value.astype(BF16)
        chain(d, p, i).start()

    dcut = cut(width, 384)
    ucut = cut(width, 768)

    def grad_in(i):
        here = pl.ds(i * dcut, dcut)
        out = contract_first(norm[:, here], gu[...]).astype(BF16)
        for b in range(blocks):
            at = pl.ds(b * LANE, LANE)
            ggate_ref[here, at] = out[:, 2 * b * LANE : (2 * b + 1) * LANE]
            gup_ref[here, at] = out[:, (2 * b + 1) * LANE : (2 * b + 2) * LANE]

    def grad_out(i):
        here = pl.ds(i * ucut, ucut)
        gdown_ref[:, here] = contract_first(hid[...], tok[1, :, here]).astype(BF16)

    fill = [functools.partial(grad_in, i) for i in range(width // dcut)]
    fill += [functools.partial(grad_out, i) for i in range(width // ucut)]

    for g in (1, 0):
        for p in range(2):
            share(g, p).wait_recv()
    for d in range(2):
        for p in range(2):
            pass_on(d, p, 1)
    gain_side.wait_recv()
    for d in range(2):
        gring[d, 0] = gg[core] + ggin[...]
    gain_count = (half, half - 1)
    for d in range(2):
        gain_hop(d, 1).start()

    done = 0
    for i in range(1, half + 1):
        upto = len(fill) * i // half
        for work in fill[done:upto]:
            work()
        done = upto
        for d in range(2):
            for p in range(2):
                if i <= hops(d, p):
                    chain(d, p, i).wait_recv()
                    if i < hops(d, p):
                        pass_on(d, p, i + 1)
        for d in range(2):
            if i <= gain_count[d]:
                gain_hop(d, i).wait_recv()
                if i < gain_count[d]:
                    gain_hop(d, i + 1).start()

    gain_sum = gring[0, 0]
    for d in range(2):
        for i in range(1, gain_count[d] + 1):
            gain_sum = gain_sum + gring[d, i]
    ggend[core] = gain_sum
    gain_back = pltpu.make_async_remote_copy(
        src_ref=ggend.at[core], dst_ref=ggend.at[core], send_sem=gx_send.at[1], recv_sem=gx_recv.at[1],
        device_id=partner, device_id_type=MESH,
    )
    gain_back.start()

    at = span(0, 0)
    sc = scale[at, 0:1]
    unit_rows = tok[0, at, :].astype(F32) * sc
    unit_grad = []
    for p in range(2):
        value = total(0, p)
        for d in range(2):
            value = value + rbuf[d, p, hops(d, p) - 1].astype(F32)
        unit_grad.append(value * gain_ref[:, cols(p)])
    sums = 0.0
    for p in range(2):
        sums = sums + jnp.sum(unit_grad[p] * unit_rows[:, p * hw : (p + 1) * hw], axis=1, keepdims=True)
    inner_mean = sums / width
    for p in range(2):
        unit = unit_rows[:, p * hw : (p + 1) * hw]
        gres_ref[:, cols(p)] = (
            tok[1, at, cols(p)].astype(F32) + sc * (unit_grad[p] - unit * inner_mean)
        ).astype(BF16)

    for a in range(2):
        for d in range(2):
            for p in range(2):
                for s in range(1, hops(d, p) + 1):
                    ring_copy(a, d, p, s).wait_send()
        for slot in range(chips):
            side_copy(a, slot).wait_send()
    for g in range(2):
        for p in range(2):
            share(g, p).wait_send()
    for d in range(2):
        for p in range(2):
            for i in range(1, hops(d, p) + 1):
                chain(d, p, i).wait_send()
        for i in range(1, gain_count[d] + 1):
            gain_hop(d, i).wait_send()
    gain_side.wait_send()
    gain_back.wait()
    ggain_ref[...] = ggend[...]


def per_device(chips, residual, upstream, gate_weight, up_weight, down_weight, gain):
    rows, width = residual.shape
    units = gate_weight.shape[1]
    half = chips // 2
    hw = width // 2
    group = chips // 2
    all_rows = 2 * chips * rows
    vmem = pl.BlockSpec(memory_space=pltpu.VMEM)
    anywhere = pl.BlockSpec(memory_space=pl.ANY)
    dma = pltpu.SemaphoreType.DMA
    outs = pl.pallas_call(
        functools.partial(kernel, chips, rows, width, units),
        out_shape=(
            jax.ShapeDtypeStruct((rows, width), BF16),
            jax.ShapeDtypeStruct((width, units), BF16),
            jax.ShapeDtypeStruct((width, units), BF16),
            jax.ShapeDtypeStruct((units, width), BF16),
            jax.ShapeDtypeStruct((2, 1, hw), F32),
        ),
        in_specs=[anywhere] * 5 + [vmem],
        out_specs=(vmem,) * 5,
        scratch_shapes=[
            pltpu.VMEM((2, all_rows, width), BF16),
            pltpu.VMEM((all_rows, width), BF16),
            pltpu.VMEM((all_rows, LANE), F32),
            pltpu.VMEM((width, 2 * units), BF16),
            pltpu.VMEM((units, width), BF16),
            pltpu.VMEM((all_rows // 2, units), F32),
            pltpu.VMEM((all_rows // 2, units), F32),
            pltpu.VMEM((all_rows, 2 * units), BF16),
            pltpu.VMEM((all_rows, units), BF16),
            pltpu.VMEM((2, 2, group * rows, hw), F32),
            pltpu.VMEM((2, 2, group * rows, hw), BF16),
            pltpu.VMEM((2, 2, group * rows, hw), BF16),
            pltpu.VMEM((2, 2, half, rows, hw), BF16),
            pltpu.VMEM((2, 2, half, rows, hw), BF16),
            pltpu.VMEM((2, 1, hw), F32),
            pltpu.VMEM((1, hw), F32),
            pltpu.VMEM((2, half + 1, 1, hw), F32),
            pltpu.VMEM((2, 1, hw), F32),
            dma((2 * units // LANE + 1,)),
            dma((2,)),
            dma((2, 2, half)),
            dma((2, 2, half)),
            dma((2, 2, 2, half)),
            dma((2, 2, 2, half)),
            dma((2, chips)),
            dma((2, chips)),
            dma((2, 2)),
            dma((2, 2)),
            dma((2, half)),
            dma((2, half)),
            dma((2,)),
            dma((2,)),
        ],
        compiler_params=pltpu.CompilerParams(
            collective_id=0, has_side_effects=True, vmem_limit_bytes=VMEM_LIMIT
        ),
        name="ffn_backward",
    )(residual, upstream, gate_weight, up_weight, down_weight, gain.reshape(1, width))
    grad_residual, grad_gate, grad_up, grad_down, grad_gain = outs
    return grad_residual, grad_gate, grad_up, grad_down, grad_gain.reshape(width)


VMEM_LIMIT = 40 * 1024 * 1024


def solution(mesh):
    both = P(("member", "dp"), None)
    split = P("member", "dp")
    return jax.shard_map(
        functools.partial(per_device, mesh.shape["dp"] // 2),
        mesh=mesh,
        in_specs=(both, both, split, split, both, P("member")),
        out_specs=(both, split, split, both, P("member")),
        check_vma=False,
    )
```
